16 devices in a mesh: dp: 2 (over y, z), tp: 8 (over x, core).
Axes of the slice: x: 4, y: 2, z: 1, core: 2. Of those that a mesh axis runs over, the one named last changes fastest.
The devices are a block of a 4x4x8 slice.
Arguments:
- x: bfloat16 [4096, 14336], P('dp'), parts along dimension 0
- gain: bfloat16 [14336], replicated
- wq: bfloat16 [14336, 14336], P(None, 'tp')
- wk: bfloat16 [14336, 14336], P(None, 'tp')
- wv: bfloat16 [14336, 14336], P(None, 'tp')
- wo: bfloat16 [14336, 14336], P('tp')
Outputs:
- output: bfloat16 [4096, 14336], P('dp'), parts along dimension 0
There are 2 independent parts. The reference program is written for one: setup_inputs(seed, part) draws one part's arguments, and reference() takes and returns one part's arrays. A program takes and returns all parts, laid end to end along the dimension named above; an argument that names none is the same for every part.
All inputs are finite; a program needn't handle non-finite values.
Results may differ from the reference program's by a relative error of at most 0.012.
Values are sent between devices in bfloat16 or wider.
A program may use at most 768 MiB of HBM per device.

```python
import jax
import jax.numpy as jnp
from jax import lax

ROWS = 2048
D = 14336
HEADS = 112
KV_HEADS = 112
HEAD = 128
THETA = 10000


def setup_inputs(seed: int = 0, part: int = 0) -> dict:
    kx, kn, kq, kk, kv, ko = jax.random.split(jax.random.key(seed), 6)

    def weights(key, rows, columns):
        return jax.random.normal(key, (rows, columns), jnp.float32) * rows**-0.5

    drawn = {
        "x": jax.random.normal(jax.random.fold_in(kx, part), (ROWS, D), jnp.float32),
        "gain": 1 + 0.1 * jax.random.normal(kn, (D,), jnp.float32),
        "wq": 2 * weights(kq, D, HEADS * HEAD),
        "wk": 2 * weights(kk, D, KV_HEADS * HEAD),
        "wv": 4 * weights(kv, D, KV_HEADS * HEAD),
        "wo": weights(ko, HEADS * HEAD, D),
    }
    return {k: v.astype(jnp.bfloat16) for k, v in drawn.items()}


def normed(x, gain):
    wide = x.astype(jnp.float32)
    scale = lax.rsqrt(jnp.mean(wide * wide, -1, keepdims=True) + 1e-6)
    return (wide * scale * gain.astype(jnp.float32)).astype(jnp.bfloat16)


def turned(t, place, theta):
    half = t.shape[-1] // 2
    angle = place.astype(jnp.float32)[:, None] * theta ** (-jnp.arange(half, dtype=jnp.float32) / half)
    cos, sin = jnp.cos(angle)[:, None], jnp.sin(angle)[:, None]
    a, b = t[..., :half].astype(jnp.float32), t[..., half:].astype(jnp.float32)
    return jnp.concatenate([a * cos - b * sin, b * cos + a * sin], -1).astype(jnp.bfloat16)


def matmul(a, w):
    return jnp.dot(a, w, preferred_element_type=jnp.float32).astype(jnp.bfloat16)


def einsum(form, a, b):
    return jnp.einsum(form, a.astype(jnp.float32), b.astype(jnp.float32))


def attention(q, k, v):
    scores = einsum("tgsd,ugd->gstu", q, k) * q.shape[-1] ** -0.5
    token = jnp.arange(q.shape[0])
    scores = jnp.where(token[:, None] >= token, scores, -jnp.inf)
    weights = jax.nn.softmax(scores, -1).astype(jnp.bfloat16)
    return einsum("gstu,ugd->tgsd", weights, v).astype(jnp.bfloat16)


def reference(x, gain, wq, wk, wv, wo):
    a, place = normed(x, gain), jnp.arange(ROWS)
    q = turned(matmul(a, wq).reshape(ROWS, HEADS, HEAD), place, THETA).reshape(ROWS, KV_HEADS, -1, HEAD)
    k = turned(matmul(a, wk).reshape(ROWS, KV_HEADS, HEAD), place, THETA)
    v = matmul(a, wv).reshape(ROWS, KV_HEADS, HEAD)
    seen = attention(q, k, v).reshape(ROWS, HEADS * HEAD)
    return (x.astype(jnp.float32) + jnp.dot(seen, wo, preferred_element_type=jnp.float32)).astype(jnp.bfloat16)
```

```python
import functools

import jax
import jax.numpy as jnp
from jax import lax
from jax.experimental import pallas as pl
from jax.experimental.pallas import tpu as pltpu
from jax.sharding import PartitionSpec as P


NEG = -1e30
HIDDEN = 2 * NEG
LOG2E = 1.4426950408889634
HEAD = 128
THETA = 10000
VMEM = 56 * 2**20
CHUNKS = ((512,), (512,), (512,), (384,), (128,))
STEADY = ((1, "turn"), (2, "start"), (2, "turn"), (2, "out"))
PLACES = (STEADY, STEADY, STEADY, ((1, "out"),), ())
SLAB = 32


def _dot(a, b, ca, cb):
    return lax.dot_general(a, b, (((ca,), (cb,)), ((), ())), preferred_element_type=jnp.float32)


def _attention(q_ref, k_ref, v_ref, o_ref, top_s, mix_s, gap_s, *, start, bq, bk, heads, scale):
    iq, c = pl.program_id(0), pl.program_id(1)
    e = scale * LOG2E
    first = start + iq * bq
    head = lambda h: slice(h * HEAD, (h + 1) * HEAD)

    @pl.when(c == 0)
    def _():
        gap_s[...] = lax.broadcasted_iota(jnp.int32, (bk, bq), 1) - lax.broadcasted_iota(jnp.int32, (bk, bq), 0)
        top_s[...] = jnp.full(top_s.shape, NEG, jnp.float32)
        mix_s[...] = jnp.zeros(mix_s.shape, jnp.float32)

    ones = jnp.ones((8, bk), jnp.bfloat16)

    def block(masked):
        scores = [_dot(k_ref[:, head(h)], q_ref[:, head(h)], 1, 1) for h in range(heads)]
        ok = gap_s[...] >= c * bk - first if masked else None
        weights, keeps = [], []
        for h, s in enumerate(scores):
            if masked:
                s = jnp.where(ok, s, HIDDEN)
            old = top_s[h : h + 1, :]
            top = jnp.maximum(old, s.max(axis=0, keepdims=True))
            top_s[h : h + 1, :] = top
            weights.append(jnp.exp2((s - top) * e).astype(jnp.bfloat16))
            keeps.append(jnp.exp2((old - top) * e))
        for h, (p, keep) in enumerate(zip(weights, keeps)):
            values = jnp.concatenate([v_ref[:, head(h)].T, ones], axis=0)
            mix_s[h] = mix_s[h] * keep + _dot(values, p, 1, 0)

    whole = (c + 1) * bk <= first + 1

    @pl.when(whole)
    def _():
        block(False)

    @pl.when(jnp.logical_not(whole) & (c * bk < first + bq))
    def _():
        block(True)

    @pl.when(c == pl.num_programs(1) - 1)
    def _():
        for h in range(heads):
            o_ref[:, head(h)] = (mix_s[h, :HEAD, :] * (1 / mix_s[h, HEAD : HEAD + 1, :])).T.astype(o_ref.dtype)


def attention(q, k, v, start, off, rows):
    width = q.shape[1]
    heads = width // HEAD
    bq, bk = 256 if rows % 256 == 0 else rows, max(n for n in (128, 256, 384, 512) if (start + rows) % n == 0)
    blocks = -(-(start + rows) // bk)
    seen = lambda i, c: (jnp.minimum(c, (start + i * bq + bq - 1) // bk), 0)
    area = rows * (start + rows // 2)
    return pl.pallas_call(
        functools.partial(_attention, start=start, bq=bq, bk=bk, heads=heads, scale=HEAD**-0.5),
        grid=(rows // bq, blocks),
        in_specs=[pl.BlockSpec((bq, width), lambda i, c: (i + off // bq, 0)), pl.BlockSpec((bk, width), seen), pl.BlockSpec((bk, width), seen)],
        out_specs=pl.BlockSpec((bq, width), lambda i, c: (i, 0)),
        out_shape=jax.ShapeDtypeStruct((rows, width), jnp.bfloat16),
        scratch_shapes=[pltpu.VMEM((heads, bq), jnp.float32), pltpu.VMEM((heads, HEAD + 8, bq), jnp.float32), pltpu.VMEM((bk, bq), jnp.int32)],
        compiler_params=pltpu.CompilerParams(dimension_semantics=("arbitrary", "arbitrary"), vmem_limit_bytes=VMEM),
        cost_estimate=pl.CostEstimate(flops=8 * heads * area * HEAD, transcendentals=heads * area, bytes_accessed=4 * q.size + 4 * (start + rows) * width),
        name="attention",
    )(q, k, v)


def _put(at, row_ref, pieces, out_ref, slab_s, in_sem, out_sem):
    slabs = [(p, row) for p, t in enumerate(pieces) for row in range(0, t.shape[0], SLAB)]
    each = slab_s.shape[1]
    groups = [slabs[n : n + each] for n in range(0, len(slabs), each)]

    def fetch(g):
        return [pltpu.make_async_copy(pieces[p].at[pl.ds(row, SLAB)], slab_s.at[g % 2, j], in_sem.at[g % 2, j]) for j, (p, row) in enumerate(groups[g])]

    def store(g):
        return [pltpu.make_async_copy(slab_s.at[g % 2, j], out_ref.at[pl.ds(pl.multiple_of(row_ref[p] + row, 8), SLAB)], out_sem.at[g % 2, j])
                for j, (p, row) in enumerate(groups[g])]

    def step(s):
        if 0 <= s - 1 < len(groups):
            for copy_in, copy_out in zip(fetch(s - 1), store(s - 1)):
                copy_in.wait()
                copy_out.start()
        if 0 <= s - 2 < len(groups):
            for copy in store(s - 2):
                copy.wait()
        if s < len(groups):
            for copy in fetch(s):
                copy.start()

    for s in range(len(groups) + 2):
        pl.when(at == s)(functools.partial(step, s))


def _projected(x_ref, scale_ref, gain_ref, wq_ref, wk_ref, wv_ref, cos_ref, sin_ref, *rest, pieces, before):
    at, last = pl.program_id(0), pl.num_programs(0) - 1
    if pieces:
        row_ref, arrays = rest[before], rest[before + 2 : before + 2 + pieces]
        q_ref, k_ref, v_ref, out_ref, sum_s, some_s, *put = rest[before + 2 + pieces :]
        _put(at, row_ref, arrays, out_ref, *put)
    else:
        q_ref, k_ref, v_ref, sum_s, some_s = rest[before:]
    width, tile = q_ref.shape[1], 2 * HEAD
    some_s[...] = (x_ref[...].astype(jnp.float32) * scale_ref[...] * gain_ref[...]).astype(jnp.bfloat16)

    def add(first):
        for j, w_ref in enumerate((wq_ref, wk_ref, wv_ref)):
            for n in range(0, width, tile):
                t = _dot(some_s[...], w_ref[:, n : n + tile], 1, 0)
                sum_s[j, :, n : n + tile] = t if first else sum_s[j, :, n : n + tile] + t

    @pl.when(at == 0)
    def _():
        add(True)

    @pl.when(at > 0)
    def _():
        add(False)

    @pl.when(at == last)
    def _():
        cos, sin = cos_ref[...], sin_ref[...]
        for n in range(0, width, HEAD):
            for j, o_ref in enumerate((q_ref, k_ref)):
                t = sum_s[j, :, n : n + HEAD].astype(jnp.bfloat16).astype(jnp.float32)
                o_ref[:, n : n + HEAD] = (t * cos + pltpu.roll(t, HEAD // 2, 1) * sin).astype(jnp.bfloat16)
        v_ref[...] = sum_s[2].astype(jnp.bfloat16)


def projected(x, scale, gain, wq, wk, wv, cos, sin, filled, start, size, landed=(), places=None, out=None):
    (rows, depth), width = x.shape, wq.shape[1]
    bk = 1024
    block = start // size
    weights = pl.BlockSpec((bk, width), lambda k: (k, 0))
    here = pl.BlockSpec((size, width), lambda k: (block, 0))
    angle = pl.BlockSpec((size, HEAD), lambda k: (block, 0))
    rest = pl.BlockSpec(memory_space=pl.ANY)
    like = jax.ShapeDtypeStruct((rows, width), jnp.bfloat16)
    given = [x, scale, gain, wq, wk, wv, cos, sin, *filled]
    in_specs = [pl.BlockSpec((size, bk), lambda k: (block, k)), pl.BlockSpec((size, 1), lambda k: (block, 0)), pl.BlockSpec((1, bk), lambda k: (0, k)),
                weights, weights, weights, angle, angle] + [rest] * len(filled)
    out_specs = [pl.BlockSpec((size, width), lambda k: (0, 0)), here, here]
    out_shape = [jax.ShapeDtypeStruct((size, width), jnp.bfloat16), like, like]
    scratch = [pltpu.VMEM((3, size, width), jnp.float32), pltpu.VMEM((size, bk), jnp.bfloat16)]
    aliases = {8: 1, 9: 2} if filled else {}
    if landed:
        each = pl.cdiv(sum(t.shape[0] for t in landed) // SLAB, depth // bk - 2)
        aliases[len(given) + 1] = 3
        given += [places, out, *landed]
        in_specs += [pl.BlockSpec(memory_space=pltpu.SMEM), rest] + [rest] * len(landed)
        out_specs += [rest]
        out_shape += [jax.ShapeDtypeStruct(out.shape, out.dtype)]
        scratch += [pltpu.VMEM((2, each, SLAB, out.shape[1]), out.dtype), pltpu.SemaphoreType.DMA((2, each)), pltpu.SemaphoreType.DMA((2, each))]
    return pl.pallas_call(
        functools.partial(_projected, pieces=len(landed), before=len(filled)),
        grid=(depth // bk,),
        in_specs=in_specs,
        out_specs=out_specs,
        out_shape=out_shape,
        input_output_aliases=aliases,
        scratch_shapes=scratch,
        compiler_params=pltpu.CompilerParams(dimension_semantics=("arbitrary",), vmem_limit_bytes=60 * 2**20),
        cost_estimate=pl.CostEstimate(flops=6 * size * depth * width, transcendentals=0, bytes_accessed=6 * depth * width),
        name="projected",
    )(*given)


def _term(a_ref, w_ref, o_ref):
    tile = min(512, o_ref.shape[1])
    for n in range(0, o_ref.shape[1], tile):
        o_ref[:, n : n + tile] = _dot(a_ref[...], w_ref[:, n : n + tile], 1, 0).astype(jnp.bfloat16)


def term_of(a, w):
    (rows, width), columns = a.shape, w.shape[1]
    bn = 2048
    return pl.pallas_call(
        _term,
        grid=(columns // bn,),
        in_specs=[pl.BlockSpec((rows, width), lambda j: (0, 0)), pl.BlockSpec((width, bn), lambda j: (0, j))],
        out_specs=pl.BlockSpec((rows, bn), lambda j: (0, j)),
        out_shape=jax.ShapeDtypeStruct((rows, columns), jnp.bfloat16),
        compiler_params=pltpu.CompilerParams(dimension_semantics=("arbitrary",), vmem_limit_bytes=VMEM),
        cost_estimate=pl.CostEstimate(flops=2 * rows * width * columns, transcendentals=0, bytes_accessed=2 * width * columns),
        name="term",
    )(a, w)


def angles(rows):
    half = HEAD // 2
    element = jnp.arange(HEAD) % half
    angle = jnp.arange(rows).astype(jnp.float32)[:, None] * THETA ** (-element.astype(jnp.float32) / half)
    sin = jnp.sin(angle)
    return jnp.cos(angle), jnp.where(jnp.arange(HEAD) < half, -sin, sin)


def room(shape):
    return pl.pallas_call(
        lambda o_ref: None, out_specs=pl.BlockSpec(memory_space=pl.ANY), out_shape=jax.ShapeDtypeStruct(shape, jnp.bfloat16), name="room"
    )()


def solution(mesh):
    group = mesh.shape["tp"]

    def ring(by):
        return [(i, (i + 2 * by) % group) for i in range(group)]

    other = [(i, i ^ 1) for i in range(group)]

    def travel(x, term, start, land):
        me = lax.convert_element_type(lax.axis_index("tp"), jnp.uint32)

        def send(t, pairs):
            return lax.ppermute(t, "tp", pairs)

        mine = lax.psum_scatter(term, "tp", scatter_dimension=0, tiled=True)
        n = mine.shape[0]
        own = lax.dynamic_slice_in_dim(x, start + lax.convert_element_type(me, jnp.int32) * n, n)
        mine = (own.astype(jnp.float32) + mine.astype(jnp.float32)).astype(jnp.bfloat16)
        land(mine, start, n, 0, 0)
        yield mine
        right, left, pair = send(mine, ring(1)), send(mine, ring(-1)), send(mine, other)
        land(pair, start, n, 0, 1)
        land(right, start, n, -1, 0)
        land(left, start, n, 1, 0)
        yield right, left, pair
        far_r, far_l = send(right[: n // 2], ring(1)), send(left[n // 2 :], ring(-1))
        pair_r, pair_l = send(right, other), send(left, other)
        land(pair_r, start, n, -1, 1)
        land(pair_l, start, n, 1, 1)
        land(far_r, start, n, -2, 0)
        land(far_l, start + n // 2, n, 2, 0)
        yield far_r, far_l, pair_r, pair_l
        pair_fr, pair_fl = send(far_r, other), send(far_l, other)
        land(pair_fr, start, n, -2, 1)
        land(pair_fl, start + n // 2, n, 2, 1)
        yield pair_fr, pair_fl

    def step(x, gain, wq, wk, wv, wo):
        rows = x.shape[0]
        cos, sin = angles(rows)
        gain32 = gain.astype(jnp.float32)[None]
        out = room(x.shape)

        landed = []

        def land(t, row, n, by, swap):
            landed.append((t, row, n, by, swap))

        def rows_of(row, n, by, swap):
            me = lax.convert_element_type(lax.axis_index("tp"), jnp.uint32)
            by = jnp.asarray(by, jnp.int32) * 2 + group
            owner = lax.rem(me + by.astype(jnp.uint32), jnp.uint32(group)) ^ jnp.asarray(swap, jnp.uint32)
            return jnp.asarray(row, jnp.int32) + owner.astype(jnp.int32) * jnp.asarray(n, jnp.int32)

        going = []

        def wait(t, chunk, place):
            for entry in going:
                since, trip, places = entry
                if places and places[0] == (chunk - since, place):
                    places.pop(0)
                    got = next(trip, None)
                    if got is not None:
                        t, _ = lax.optimization_barrier((t, got))
            return t

        start = part = 0
        filled = []
        for parts in CHUNKS:
            size = sum(parts)
            wide = x.astype(jnp.float32)
            scale = lax.rsqrt(jnp.mean(wide * wide, -1, keepdims=True) + 1e-6)
            gain_i = wait(gain32, part, "start")
            some, at = [], None
            if landed:
                some, *at = zip(*landed)
                at = rows_of(*at)
                landed.clear()
            q, *filled = projected(x, scale, gain_i, wq, wk, wv, cos, sin, filled, start, size, some, at, out)
            if some:
                out = filled.pop()
            off = 0
            for n in parts:
                seen = attention(wait(q, part, "turn"), *filled, start + off, off, n)
                term = term_of(wait(seen, part, "out"), wo)
                going.append((part, travel(x, term, start + off, land), list(PLACES[part])))
                off += n
                part += 1
            start += size
        for _, trip, _ in going:
            for _ in trip:
                pass
        out, _ = lax.optimization_barrier((out, term))
        for t, *at in landed:
            out = lax.dynamic_update_slice(out, t, (rows_of(*at), 0))
        return out

    tokens, columns = P("dp", None), P(None, "tp")
    return jax.shard_map(
        step,
        mesh=mesh,
        in_specs=(tokens, P(None), columns, columns, columns, P("tp", None)),
        out_specs=tokens,
        check_vma=False,
    )
```
